32 devices in a mesh: section: 4 (over y, x), dp: 4 (over z), tensor: 2 (over core).
Axes of the slice: x: 2, y: 2, z: 4, core: 2. Of those that a mesh axis runs over, the one named last changes fastest.
Arguments:
- activations: bfloat16 [512, 8192], P('dp', 'tensor'), may hold values from -6 to 6
- targets: bfloat16 [4, 512, 8192], P('section', 'dp', 'tensor'), may hold values from -12 to 12
- packed_floors: int32 [4, 2048, 8192], P('section', 'dp', 'tensor'), may hold values from 0 to 4095
- rounding: float32 [4, 8192, 8192], P('section', 'dp', 'tensor'), may hold values from -8 to 8
- scales: float32 [4, 8192], P('section', 'tensor'), may hold values from 0.001 to 0.006
- norm_gains: float32 [4, 8192], P('section'), may hold values from 0.5 to 1.5
Outputs:
- rounding_next: float32 [4, 8192, 8192], P('section', 'dp', 'tensor')
- block_outputs: bfloat16 [4, 512, 8192], P('section', 'dp', 'tensor')
- losses: float32 [4], P('section')
The draws below stay inside these ranges and needn't reach their ends.
Inputs may be any that keep to these rules, and one draw needn't show every extreme that they name: `packed_floors`: each word holds four 3-bit codes in its lowest 12 bits, lowest bits first: code k of word r of a column is row 4 r + k; the floor is the code minus 4.
All inputs are finite; a program needn't handle non-finite values.
Results may differ from the reference program's by a relative error of at most 0.0045.
The reference program's roundings to bfloat16 on the way count: a program that leaves them out, or rounds other values in their place, can miss the bound.
Values may be sent and summed in bfloat16 or wider, within the bound.
A program may use at most 192 MiB of HBM per device.

```python
import math
import jax
import jax.numpy as jnp
from jax import lax

D = 8192
TOKENS = 512
N_SECTION = 4


def draw_rounding(key, part):
    key_base = jax.random.fold_in(key, 11)
    key_rows = jax.random.fold_in(key, 12)
    key_cols = jax.random.fold_in(key, 13)
    positions = jnp.arange(D, dtype=jnp.float32) / (D - 1)
    row_level = positions[None, :, None] * jnp.ones((N_SECTION, D, 1), jnp.float32)
    col_level = positions[None, None, :] * jnp.ones((N_SECTION, 1, D), jnp.float32)
    row_rough = jax.random.uniform(key_rows, (N_SECTION, D, 1), jnp.float32, 0.6, 1.5)
    col_rough = jax.random.uniform(key_cols, (N_SECTION, 1, D), jnp.float32, 0.6, 1.5)
    spread = 0.15 * jnp.exp(jnp.log(40.0) * 0.5 * (row_level + col_level)) * row_rough * col_rough
    base = jax.random.normal(key_base, (N_SECTION, D, D), jnp.float32)
    return jnp.clip(base * spread, -8.0, 8.0)


def plant(drawn, rng, smallest, largest):
    place = [jax.random.randint(jax.random.fold_in(rng, axis), (), 0, length) for axis, length in enumerate(drawn.shape)]
    main_axis = drawn.shape.index(max(drawn.shape))
    next_to = place[:main_axis] + [(place[main_axis] + 1) % drawn.shape[main_axis]] + place[main_axis + 1:]
    return drawn.at[tuple(place)].set(smallest).at[tuple(next_to)].set(largest)


def level_of(rng, shape, split, low, top_value):
    def one(axis_at, blocks):
        draws = jax.random.uniform(jax.random.fold_in(jax.random.fold_in(rng, 6), axis_at), (blocks,), jnp.float32, low / len(split), top_value / len(split))
        return jnp.repeat(jnp.exp(draws), shape[axis_at] // blocks).reshape((-1,) + (1,) * (len(shape) - axis_at - 1))

    loudness = one(*split[0])
    for cut in split[1:]:
        loudness = loudness * one(*cut)
    return loudness


def gaussian(own_key, dims, scale, most, pieces=(), held_as=jnp.bfloat16):
    array = scale * jax.random.normal(own_key, dims, jnp.float32)
    if pieces:
        array = array * level_of(own_key, dims, pieces, -0.22, 0.18)
    return jnp.clip(array, -most, most).astype(held_as)


def setup_inputs(seed: int = 0) -> dict:
    streams_of = jax.random.split(jax.random.key(seed), 7)
    activations = gaussian(streams_of[0], (TOKENS, D), 1.0, 6.0, ((0, 4), (1, 2)))
    targets = gaussian(streams_of[1], (N_SECTION, TOKENS, D), 2.0, 12.0, ((0, 4), (1, 4), (2, 2)))
    packed_floors = plant(jax.random.randint(streams_of[2], (N_SECTION, D // 4, D), 0, 4096), jax.random.fold_in(streams_of[2], 1), 0, 4095).astype(jnp.int32)
    rounding = draw_rounding(jax.random.fold_in(streams_of[6], 71), 0)
    scales = jnp.clip(jnp.exp(math.log(0.006) - 1.7917594 * jax.random.uniform(streams_of[4], (N_SECTION, D), jnp.float32) ** level_of(streams_of[4], (N_SECTION, D), ((0, 4), (1, 2)), -0.2, 0.2)), 0.001, 0.006)
    norm_gains = jnp.clip(1.0 + 0.1 * jax.random.normal(streams_of[5], (N_SECTION, D), jnp.float32), 0.5, 1.5)
    return {"activations": activations, "targets": targets, "packed_floors": packed_floors, "rounding": rounding, "scales": scales, "norm_gains": norm_gains}


norm_eps = 1e-06
grad_eps = 1e-06
reg_weight = 0.3
step_rate = 0.25
error_scale = 600.0

def unpack(words):
    shifts = 3 * jnp.arange(4, dtype=jnp.int32)
    codes = jnp.right_shift(words[:, None, :], shifts[None, :, None]) & 7
    return codes.reshape(words.shape[0] * 4, words.shape[1]).astype(jnp.float32) - 4.0

def soft_round(values):
    sig = jax.nn.sigmoid(values)
    linear = 1.2 * sig - 0.1
    soft_part = jnp.clip(linear, 0.0, 1.0)
    soft_slope = jnp.where((linear > 0.0) & (linear < 1.0), 1.2 * sig * (1.0 - sig), 0.0)
    return (soft_part, soft_slope)

def reference(activations, targets, packed_floors, rounding, scales, norm_gains):
    token_total, width_full = activations.shape
    current = activations
    next_list, output_list, loss_list = ([], [], [])
    for section_index in range(N_SECTION):
        floors = unpack(packed_floors[section_index])
        soft_part, soft_slope = soft_round(rounding[section_index])
        weight = (scales[section_index][None, :] * (floors + soft_part)).astype(jnp.bfloat16)
        inputs = current.astype(jnp.float32)
        mean_sq = lax.optimization_barrier(jnp.mean(inputs * inputs, axis=1, keepdims=True))
        normed = (inputs * lax.rsqrt(mean_sq + norm_eps) * norm_gains[section_index][None, :]).astype(jnp.bfloat16)
        result = (inputs + jnp.dot(normed, weight, preferred_element_type=jnp.float32)).astype(jnp.bfloat16)
        residue = result.astype(jnp.float32) - targets[section_index].astype(jnp.float32)
        delta = (error_scale / token_total ** 0.5 * residue).astype(jnp.bfloat16)
        grad_w = lax.dot_general(normed, delta, (((0,), (0,)), ((), ())), preferred_element_type=jnp.float32)
        polarity = 2.0 * soft_part - 1.0
        grad = soft_slope * (scales[section_index][None, :] * grad_w - 8.0 * reg_weight * polarity ** 3)
        mean_grad = jnp.sum(grad * grad) / (width_full * width_full) + grad_eps
        next_list.append(rounding[section_index] - step_rate * grad * lax.rsqrt(mean_grad))
        loss_list.append(jnp.sum(residue * residue) / (token_total * width_full) + reg_weight * jnp.sum(1.0 - polarity ** 4) / (width_full * width_full))
        output_list.append(result)
        current = result
    return (jnp.stack(next_list), jnp.stack(output_list), jnp.stack(loss_list))
```

```python
import functools
import jax
import jax.numpy as jnp
from jax import lax
from jax.experimental import pallas as pl
from jax.experimental.pallas import tpu as pltpu
from jax.sharding import PartitionSpec as P

MICRO = 4
SPLIT = 4


norm_eps = 1e-06
grad_eps = 1e-06
reg_weight = 0.3
step_rate = 0.25
error_scale = 600.0

VMEM_ALL = 62 * 1024 * 1024


def tile_of(size, most):
    while size % most:
        most //= 2
    return most


def weight_kernel(packed_ref, rounding_ref, scale_ref, weight_ref):
    rows, cols = rounding_ref.shape
    strip_c = tile_of(cols, 512)
    strip_r = 32

    @pl.loop(0, cols // strip_c)
    def _(cb):
        col = pl.ds(pl.multiple_of(cb * strip_c, strip_c), strip_c)
        scale = scale_ref[:, col]
        shift = 3 * (lax.broadcasted_iota(jnp.int32, (strip_r, strip_c), 0) & 3)

        @pl.loop(0, rows // strip_r)
        def _(rb):
            row = pl.ds(pl.multiple_of(rb * strip_r, strip_r), strip_r)
            word = pl.ds(pl.multiple_of(rb * (strip_r // 4), strip_r // 4), strip_r // 4)
            words = jnp.repeat(packed_ref[word, col], 4, axis=0)
            codes = (jnp.right_shift(words, shift) & 7).astype(jnp.float32)
            half = jnp.tanh(0.5 * rounding_ref[row, col])
            soft = jnp.clip(0.6 * half + 0.5, 0.0, 1.0)
            weight_ref[row, col] = (scale * ((codes - 4.0) + soft)).astype(jnp.bfloat16)


def make_weight(packed, rounding, scale_row):
    rows, cols = rounding.shape
    tr, tc = tile_of(rows, 256), tile_of(cols, 2048)
    return pl.pallas_call(
        weight_kernel,
        out_shape=jax.ShapeDtypeStruct((rows, cols), jnp.bfloat16),
        grid=(cols // tc, rows // tr),
        in_specs=[
            pl.BlockSpec((tr // 4, tc), lambda j, i: (i, j)),
            pl.BlockSpec((tr, tc), lambda j, i: (i, j)),
            pl.BlockSpec((1, tc), lambda j, i: (0, j)),
        ],
        out_specs=pl.BlockSpec((tr, tc), lambda j, i: (i, j)),
        compiler_params=pltpu.CompilerParams(dimension_semantics=("arbitrary", "arbitrary")),
        cost_estimate=pl.CostEstimate(
            flops=20 * rows * cols, transcendentals=rows * cols, bytes_accessed=7 * rows * cols
        ),
    )(packed, rounding, scale_row)


def grad_kernel(rows_ref, delta_ref, rounding_ref, scale_ref, grad_ref, sums_ref, product):
    trow, tcol = rounding_ref.shape
    strip_c = tile_of(tcol, 512)
    strip_r = 16
    first = (pl.program_id(0) == 0) & (pl.program_id(1) == 0)

    @pl.when(first)
    def _():
        sums_ref[...] = jnp.zeros_like(sums_ref)

    product[...] = lax.dot_general(
        rows_ref[...], delta_ref[...], (((0,), (0,)), ((), ())), preferred_element_type=jnp.float32
    )

    @pl.loop(0, tcol // strip_c)
    def _(cb):
        col = pl.ds(pl.multiple_of(cb * strip_c, strip_c), strip_c)
        scale = scale_ref[:, col]

        def strip(rb, sums):
            row = pl.ds(pl.multiple_of(rb * strip_r, strip_r), strip_r)
            full = 1.2 * jnp.tanh(0.5 * rounding_ref[row, col])
            inside = jnp.abs(full) < 1.0
            polarity = jnp.clip(full, -1.0, 1.0)
            square = polarity * polarity
            slope = jnp.where(inside, 0.3 - (0.3 / 1.44) * square, 0.0)
            grad = slope * (scale * product[row, col] - (8.0 * reg_weight) * (square * polarity))
            grad_ref[row, col] = grad.astype(grad_ref.dtype)
            fold = lambda v: v.reshape(strip_r // 8, 8, strip_c).sum(axis=0)
            return sums[0] + fold(grad * grad), sums[1] + fold(1.0 - square * square)

        zero = jnp.zeros((8, strip_c), jnp.float32)
        grads, pens = lax.fori_loop(0, trow // strip_r, strip, (zero, zero))
        lanes = lambda v: sum(v[:, k : k + 128] for k in range(0, strip_c, 128))
        sums_ref[0] += lanes(grads)
        sums_ref[1] += lanes(pens)


def make_grad(rows_all, delta_all, rounding, scale_row):
    tokens, rows = rows_all.shape
    cols = delta_all.shape[1]
    tr, tc = tile_of(rows, 256), tile_of(cols, 2048)
    return pl.pallas_call(
        grad_kernel,
        out_shape=(
            jax.ShapeDtypeStruct((rows, cols), jnp.bfloat16),
            jax.ShapeDtypeStruct((2, 8, 128), jnp.float32),
        ),
        grid=(cols // tc, rows // tr),
        in_specs=[
            pl.BlockSpec((tokens, tr), lambda j, i: (0, i)),
            pl.BlockSpec((tokens, tc), lambda j, i: (0, j)),
            pl.BlockSpec((tr, tc), lambda j, i: (i, j)),
            pl.BlockSpec((1, tc), lambda j, i: (0, j)),
        ],
        out_specs=(
            pl.BlockSpec((tr, tc), lambda j, i: (i, j)),
            pl.BlockSpec((2, 8, 128), lambda j, i: (0, 0, 0)),
        ),
        scratch_shapes=[pltpu.VMEM((tr, tc), jnp.float32)],
        compiler_params=pltpu.CompilerParams(dimension_semantics=("arbitrary", "arbitrary")),
        cost_estimate=pl.CostEstimate(
            flops=2 * tokens * rows * cols, transcendentals=rows * cols, bytes_accessed=6 * rows * cols
        ),
    )(rows_all, delta_all, rounding, scale_row)


def chain_kernel(
    act_ref, target_ref, weight_hbm, gain_ref, gain_next_ref,
    out_ref, residue_ref, rows_hbm, delta_hbm,
    weight, rows, part, own, landed, carried, normed, normed0, stat, delta,
    w_sem, row_sem, relay_sem, part_send, part_recv, carry_sem, carry_recv,
    norm_send, norm0_send, stat_send, stat_recv, delta_send, delta_recv, store_sem,
):
    section, z, t = (lax.axis_index(name) for name in ("section", "dp", "tensor"))
    sections, dp, nt = (lax.axis_size(name) for name in ("section", "dp", "tensor"))
    micro, _, tok, depth = rows.shape
    cols = out_ref.shape[1]
    pieces = cols // depth
    wide = cols // SPLIT
    model = depth * dp
    first = section == 0
    inner = section < sections - 1

    def remote(src, dst, send, recv, s, d, c):
        return pltpu.make_async_remote_copy(
            src_ref=src, dst_ref=dst, send_sem=send, recv_sem=recv,
            device_id={"section": s, "dp": d, "tensor": c}, device_id_type=pl.DeviceIdType.MESH,
        )

    def arrived(dst, recv):
        remote(dst, dst, recv, recv, section, z, t).wait_recv()

    def left(src, send):
        remote(src, src, send, send, section, z, t).wait_send()

    def columns(q):
        return pl.ds(q * wide, wide)

    def weight_copy(q):
        return pltpu.make_async_copy(
            weight_hbm.at[:, columns(q)], weight.at[:, columns(q)], w_sem.at[q]
        )

    for q in range(SPLIT):
        weight_copy(q).start()

    def token_rows(m):
        return pl.ds(m * tok, tok)

    def stat_start(kind, m, total):
        stat[kind, m, t] = jnp.broadcast_to(total, (tok, 128))
        for k in range(1, nt):
            remote(
                stat.at[kind, m, t], stat.at[kind, m, t], stat_send.at[kind, m, k], stat_recv.at[kind, m, t],
                section, z, lax.rem(t + k, nt),
            ).start()

    def inverse(kind, m):
        for k in range(1, nt):
            other = lax.rem(t + k, nt)
            arrived(stat.at[kind, m, other], stat_recv.at[kind, m, other])
        total = stat[kind, m, 0][:, :1]
        for k in range(1, nt):
            total = total + stat[kind, m, k][:, :1]
        return lax.rsqrt(total / model + norm_eps)

    entry = lax.rem(z, nt)

    def at_home(c):
        return first & (t * pieces + c == z) & (entry == t)

    def norm_copy(m, c, initial):
        buf, sem = (normed0, norm0_send) if initial else (normed, norm_send)
        return remote(
            buf.at[m, c], rows.at[m, z], sem.at[m, c], row_sem.at[m, z],
            section if initial else section + 1, t * pieces + c, entry,
        )

    def spread(m, src, gain, initial):
        inv = inverse(0 if initial else 1, m)
        buf = normed0 if initial else normed
        for c in range(pieces):
            cut = pl.ds(c * depth, depth)
            value = (src[token_rows(m), cut].astype(jnp.float32) * inv * gain[:, cut]).astype(jnp.bfloat16)
            buf[m, c] = value
            if initial:

                @pl.when(at_home(c))
                def _():
                    rows[m, z] = value

                @pl.when(jnp.logical_not(at_home(c)))
                def _():
                    norm_copy(m, c, True).start()
            else:
                norm_copy(m, c, False).start()

    @pl.when(first)
    def _():
        for m in range(micro):
            value = act_ref[token_rows(m), :]
            carried[m] = value
            value = value.astype(jnp.float32)
            stat_start(0, m, jnp.sum(value * value, axis=1, keepdims=True))
        for m in range(micro):
            spread(m, act_ref, gain_ref, True)

    home_piece = lax.rem(z, pieces)
    is_sender = t == z // pieces

    def relay(m, o, k):
        return remote(
            rows.at[m, o], rows.at[m, o], relay_sem.at[m, o, k], row_sem.at[m, o],
            section, z, lax.rem(t + k, nt),
        )

    def receive_rows(m):
        for o in range(dp):
            local = first & (z == o) & is_sender

            @pl.when((t == o % nt) & jnp.logical_not(local))
            def _():
                arrived(rows.at[m, o], row_sem.at[m, o])

            @pl.when(t == o % nt)
            def _():
                for k in range(1, nt):
                    relay(m, o, k).start()

        for o in range(dp):

            @pl.when(t != o % nt)
            def _():
                arrived(rows.at[m, o], row_sem.at[m, o])

    def rows_store(m):
        return pltpu.make_async_copy(rows.at[m], rows_hbm.at[m], store_sem.at[m])

    def part_copy(m, q, k):
        to = lax.rem(z + k, dp)
        return remote(
            part.at[m, to, :, columns(q)], landed.at[m, z, :, columns(q)],
            part_send.at[m, q, k], part_recv.at[m, q, z], section, to, t,
        )

    def multiply(m):
        step = tile_of(wide, 256)
        for q in range(SPLIT):
            if m == 0:
                weight_copy(q).wait()

            @pl.loop(0, wide // step)
            def _(b):
                cut = pl.ds(pl.multiple_of(q * wide + b * step, step), step)
                value = jnp.dot(
                    rows[m].reshape(dp * tok, depth), weight[:, cut], preferred_element_type=jnp.float32
                )
                own[:, :, cut] = value.reshape(dp, tok, step)
                part[m, :, :, cut] = value.reshape(dp, tok, step).astype(jnp.bfloat16)

            for k in range(1, dp):
                part_copy(m, q, k).start()

    def hand_on(m, origin, way):
        return remote(
            delta.at[m, origin], delta.at[m, origin], delta_send.at[m, origin, way], delta_recv.at[m, origin],
            section, z + (1 if way else -1), t,
        )

    def gather_step(m, hop):
        for way in (0, 1):
            origin = z - hop if way else z + hop
            exists = (origin >= 0) & (origin < dp)
            onward = exists & ((z + 1 < dp) if way else (z >= 1))
            if hop:

                @pl.when(exists)
                def _():
                    arrived(delta.at[m, origin], delta_recv.at[m, origin])

            @pl.when(onward)
            def _():
                hand_on(m, origin, way).start()

    def finish(m):
        total = jnp.zeros((tok, 1), jnp.float32)
        squares = jnp.zeros((tok, 1), jnp.float32)

        @pl.when(jnp.logical_not(first))
        def _():
            arrived(carried.at[m], carry_recv.at[m])

        for q in range(SPLIT):
            for k in range(1, dp):
                other = lax.rem(z + k, dp)
                arrived(landed.at[m, other, :, columns(q)], part_recv.at[m, q, other])
            branch = own[z, :, columns(q)]
            for k in range(1, dp):
                branch = branch + landed[m, lax.rem(z + k, dp), :, columns(q)].astype(jnp.float32)
            value = (carried[m, :, columns(q)].astype(jnp.float32) + branch).astype(jnp.bfloat16)
            out_ref[token_rows(m), columns(q)] = value
            value = value.astype(jnp.float32)
            residue = value - target_ref[token_rows(m), columns(q)].astype(jnp.float32)
            delta[m, z, :, columns(q)] = (error_scale / (micro * dp * tok) ** 0.5 * residue).astype(jnp.bfloat16)
            total = total + jnp.sum(value * value, axis=1, keepdims=True)
            squares = squares + jnp.sum(residue * residue, axis=1, keepdims=True)
        residue_ref[token_rows(m), :] = jnp.broadcast_to(squares, (tok, 128))

        @pl.when(inner)
        def _():
            stat_start(1, m, total)
            carry_copy(m).start()
            spread(m, out_ref, gain_next_ref, False)

    def carry_copy(m):
        return remote(
            out_ref.at[token_rows(m), :], carried.at[m], carry_sem.at[m], carry_recv.at[m], section + 1, z, t
        )

    for m in range(micro):
        receive_rows(m)
        rows_store(m).start()
        multiply(m)
        finish(m)
        for hop in range(min(dp, m + 1)):
            gather_step(m - hop, hop)
    for late in range(micro, micro + dp - 1):
        for hop in range(dp):
            if 0 <= late - hop < micro:
                gather_step(late - hop, hop)
    delta_store = pltpu.make_async_copy(delta, delta_hbm, store_sem.at[micro])
    delta_store.start()

    for m in range(micro):
        for q in range(SPLIT):
            for k in range(1, dp):
                part_copy(m, q, k).wait_send()
        for o in range(dp):

            @pl.when(t == o % nt)
            def _():
                for k in range(1, nt):
                    relay(m, o, k).wait_send()

            for way in (0, 1):
                onward = ((z + 1 < dp) & (o <= z)) if way else ((z >= 1) & (o >= z))

                @pl.when(onward)
                def _():
                    hand_on(m, o, way).wait_send()

        @pl.when(first)
        def _():
            for k in range(1, nt):
                left(stat.at[0, m, t], stat_send.at[0, m, k])
            for c in range(pieces):

                @pl.when(jnp.logical_not(at_home(c)))
                def _():
                    norm_copy(m, c, True).wait_send()

        @pl.when(inner)
        def _():
            for k in range(1, nt):
                left(stat.at[1, m, t], stat_send.at[1, m, k])
            carry_copy(m).wait_send()
            for c in range(pieces):
                norm_copy(m, c, False).wait_send()

        rows_store(m).wait()
    delta_store.wait()


def run_chain(activations, targets, weight, gain_row, gain_next, dp, nt):
    tok_dev, cols = activations.shape
    depth = weight.shape[0]
    tok = tok_dev // MICRO
    pieces = cols // depth
    bf16, f32 = jnp.bfloat16, jnp.float32
    vmem = pl.BlockSpec(memory_space=pltpu.VMEM)
    hbm = pl.BlockSpec(memory_space=pl.ANY)
    dma = pltpu.SemaphoreType.DMA
    out, residue, rows_all, delta_all = pl.pallas_call(
        chain_kernel,
        out_shape=(
            jax.ShapeDtypeStruct((tok_dev, cols), bf16),
            jax.ShapeDtypeStruct((tok_dev, 128), f32),
            jax.ShapeDtypeStruct((MICRO, dp, tok, depth), bf16),
            jax.ShapeDtypeStruct((MICRO, dp, tok, cols), bf16),
        ),
        in_specs=[vmem, vmem, hbm, vmem, vmem],
        out_specs=(vmem, vmem, hbm, hbm),
        scratch_shapes=[
            pltpu.VMEM((depth, cols), bf16),
            pltpu.VMEM((MICRO, dp, tok, depth), bf16),
            pltpu.VMEM((MICRO, dp, tok, cols), bf16),
            pltpu.VMEM((dp, tok, cols), f32),
            pltpu.VMEM((MICRO, dp, tok, cols), bf16),
            pltpu.VMEM((MICRO, tok, cols), bf16),
            pltpu.VMEM((MICRO, pieces, tok, depth), bf16),
            pltpu.VMEM((MICRO, pieces, tok, depth), bf16),
            pltpu.VMEM((2, MICRO, nt, tok, 128), f32),
            pltpu.VMEM((MICRO, dp, tok, cols), bf16),
            dma((SPLIT,)),
            dma((MICRO, dp)),
            dma((MICRO, dp, nt)),
            dma((MICRO, SPLIT, dp)),
            dma((MICRO, SPLIT, dp)),
            dma((MICRO,)),
            dma((MICRO,)),
            dma((MICRO, pieces)),
            dma((MICRO, pieces)),
            dma((2, MICRO, nt)),
            dma((2, MICRO, nt)),
            dma((MICRO, dp, 2)),
            dma((MICRO, dp)),
            dma((MICRO + 1,)),
        ],
        compiler_params=pltpu.CompilerParams(has_side_effects=True, vmem_limit_bytes=VMEM_ALL),
        cost_estimate=pl.CostEstimate(
            flops=2 * tok_dev * dp * depth * cols, transcendentals=0, bytes_accessed=2 * depth * cols
        ),
    )(activations, targets, weight, gain_row, gain_next)
    return out, residue[:, 0], rows_all.reshape(-1, depth), delta_all.reshape(-1, cols)


def passed_along(value, axis, steps):
    count = lax.axis_size(axis)
    leading, last = (max(0, -steps), min(count, count - steps))
    return lax.ppermute(value, axis, [(source, source + steps) for source in range(leading, last)])


def normalize(features, gain_row):
    inputs = features.astype(jnp.float32)
    mean_sq = jnp.mean(inputs * inputs, axis=1, keepdims=True)
    return (inputs * lax.rsqrt(mean_sq + norm_eps) * gain_row[None, :]).astype(jnp.bfloat16)


def ticked_chain(activations, targets, weight, gain_row):
    section_index = lax.axis_index("section")
    section_count = lax.axis_size("section")
    dp_count = lax.axis_size("dp")
    tok_dev, width_local = activations.shape
    token_total = tok_dev * dp_count
    tok_micro = tok_dev // MICRO
    received = jnp.zeros((tok_micro, width_local), jnp.bfloat16)
    row_ticks = []
    output_ticks = []
    tick_count = MICRO + section_count - 1
    for tick_index in range(tick_count):
        fed = min(tick_index, MICRO - 1) * tok_micro
        block_input = jnp.where(section_index == 0, activations[fed : fed + tok_micro], received)
        whole_rows = lax.all_gather(block_input, "tensor", axis=1, tiled=True)
        normed = normalize(whole_rows, gain_row)
        swapped = lax.all_to_all(normed, "dp", split_axis=1, concat_axis=0, tiled=True)
        partial_value = jnp.dot(swapped, weight, preferred_element_type=jnp.float32)
        branch = lax.psum_scatter(partial_value, "dp", scatter_dimension=0, tiled=True)
        block_result = (block_input.astype(jnp.float32) + branch).astype(jnp.bfloat16)
        row_ticks.append(swapped)
        output_ticks.append(block_result)
        if tick_index + 1 < tick_count:
            received = passed_along(block_result, "section", 1)
    stored_rows = lax.dynamic_slice_in_dim(jnp.stack(row_ticks), section_index, MICRO, axis=0)
    stored_rows = stored_rows.reshape(MICRO, dp_count, tok_micro, -1).transpose(1, 0, 2, 3)
    outputs_buf = lax.dynamic_slice_in_dim(
        jnp.concatenate(output_ticks), section_index * tok_micro, tok_dev, axis=0
    )
    residue = outputs_buf.astype(jnp.float32) - targets.astype(jnp.float32)
    delta = (error_scale / token_total**0.5 * residue).astype(jnp.bfloat16)
    delta_all = lax.all_gather(delta, "dp", axis=0, tiled=True)
    rows_all = stored_rows.reshape(dp_count * tok_dev, -1)
    return outputs_buf, jnp.sum(residue * residue, axis=1), rows_all, delta_all


def per_device(activations, targets, packed_floors, rounding, scales, norm_gains):
    dp_count = lax.axis_size("dp")
    core_count = lax.axis_size("tensor")
    tok_dev, width_local = activations.shape
    width_full = norm_gains.shape[1]
    token_total = tok_dev * dp_count
    weight = make_weight(packed_floors[0], rounding[0], scales)
    if width_local % rounding.shape[1] == 0 and dp_count % core_count == 0:
        here = lax.axis_index("tensor") * width_local
        gain_row = lax.dynamic_slice_in_dim(norm_gains, here, width_local, axis=1)
        gain_next = passed_along(gain_row, "section", -1)
        outputs_buf, residues, rows_all, delta_all = run_chain(
            activations, targets[0], weight, gain_row, gain_next, dp_count, core_count
        )
    else:
        outputs_buf, residues, rows_all, delta_all = ticked_chain(
            activations, targets[0], weight, norm_gains[0]
        )
    grad, sums = make_grad(rows_all, delta_all, rounding[0], scales)
    recon_sum, penalty_sum, square_sum = lax.psum(
        (jnp.sum(residues), jnp.sum(sums[1]), jnp.sum(sums[0])), ("dp", "tensor")
    )
    mean_grad = square_sum / (width_full * width_full) + grad_eps
    rounding_next = rounding[0] - step_rate * grad.astype(jnp.float32) * lax.rsqrt(mean_grad)
    loss_value = recon_sum / (token_total * width_full) + reg_weight * penalty_sum / (
        width_full * width_full
    )
    return (rounding_next[None], outputs_buf[None], loss_value.reshape(1))


def solution(mesh):
    placed = (
        P("dp", "tensor"),
        P("section", "dp", "tensor"),
        P("section", "dp", "tensor"),
        P("section", "dp", "tensor"),
        P("section", "tensor"),
        P("section", None),
    )
    return jax.shard_map(
        per_device,
        mesh=mesh,
        in_specs=placed,
        out_specs=(P("section", "dp", "tensor"), P("section", "dp", "tensor"), P("section")),
        check_vma=False,
    )
```

```python
import functools
import jax
import jax.numpy as jnp
from jax import lax
from jax.experimental import pallas as pl
from jax.experimental.pallas import tpu as pltpu
from jax.sharding import PartitionSpec as P

MICRO = 8
TICKS = 4
SPLIT = 4


norm_eps = 1e-06
grad_eps = 1e-06
reg_weight = 0.3
step_rate = 0.25
error_scale = 600.0

VMEM_ALL = 62 * 1024 * 1024


def tile_of(size, most):
    while size % most:
        most //= 2
    return most


def weight_kernel(packed_ref, rounding_ref, scale_ref, weight_ref):
    rows, cols = rounding_ref.shape
    strip_c = tile_of(cols, 512)
    strip_r = 32

    @pl.loop(0, cols // strip_c)
    def _(cb):
        col = pl.ds(pl.multiple_of(cb * strip_c, strip_c), strip_c)
        scale = scale_ref[:, col]
        shift = 3 * (lax.broadcasted_iota(jnp.int32, (strip_r, strip_c), 0) & 3)

        @pl.loop(0, rows // strip_r)
        def _(rb):
            row = pl.ds(pl.multiple_of(rb * strip_r, strip_r), strip_r)
            word = pl.ds(pl.multiple_of(rb * (strip_r // 4), strip_r // 4), strip_r // 4)
            words = jnp.repeat(packed_ref[word, col], 4, axis=0)
            codes = (jnp.right_shift(words, shift) & 7).astype(jnp.float32)
            half = jnp.tanh(0.5 * rounding_ref[row, col])
            soft = jnp.clip(0.6 * half + 0.5, 0.0, 1.0)
            weight_ref[row, col] = (scale * ((codes - 4.0) + soft)).astype(jnp.bfloat16)


def make_weight(packed, rounding, scale_row):
    rows, cols = rounding.shape
    tr, tc = tile_of(rows, 256), tile_of(cols, 2048)
    return pl.pallas_call(
        weight_kernel,
        out_shape=jax.ShapeDtypeStruct((rows, cols), jnp.bfloat16),
        grid=(cols // tc, rows // tr),
        in_specs=[
            pl.BlockSpec((tr // 4, tc), lambda j, i: (i, j)),
            pl.BlockSpec((tr, tc), lambda j, i: (i, j)),
            pl.BlockSpec((1, tc), lambda j, i: (0, j)),
        ],
        out_specs=pl.BlockSpec((tr, tc), lambda j, i: (i, j)),
        compiler_params=pltpu.CompilerParams(dimension_semantics=("arbitrary", "arbitrary")),
        cost_estimate=pl.CostEstimate(
            flops=20 * rows * cols, transcendentals=rows * cols, bytes_accessed=7 * rows * cols
        ),
    )(packed, rounding, scale_row)


def grad_kernel(rows_ref, delta_ref, rounding_ref, scale_ref, grad_ref, sums_ref, product):
    trow, tcol = rounding_ref.shape
    strip_c = tile_of(tcol, 512)
    strip_r = 16
    first = (pl.program_id(0) == 0) & (pl.program_id(1) == 0)

    @pl.when(first)
    def _():
        sums_ref[...] = jnp.zeros_like(sums_ref)

    product[...] = lax.dot_general(
        rows_ref[...], delta_ref[...], (((0,), (0,)), ((), ())), preferred_element_type=jnp.float32
    )

    @pl.loop(0, tcol // strip_c)
    def _(cb):
        col = pl.ds(pl.multiple_of(cb * strip_c, strip_c), strip_c)
        scale = scale_ref[:, col]

        def strip(rb, sums):
            row = pl.ds(pl.multiple_of(rb * strip_r, strip_r), strip_r)
            full = 1.2 * jnp.tanh(0.5 * rounding_ref[row, col])
            polarity = jnp.clip(full, -1.0, 1.0)
            square = polarity * polarity
            slope = jnp.where(square < 1.0, 0.3 - (0.3 / 1.44) * square, 0.0)
            grad = slope * (scale * product[row, col] - (8.0 * reg_weight) * (square * polarity))
            grad_ref[row, col] = grad.astype(grad_ref.dtype)
            fold = lambda v: v.reshape(strip_r // 8, 8, strip_c).sum(axis=0)
            return sums[0] + fold(grad * grad), sums[1] + fold(1.0 - square * square)

        zero = jnp.zeros((8, strip_c), jnp.float32)
        grads, pens = lax.fori_loop(0, trow // strip_r, strip, (zero, zero))
        lanes = lambda v: sum(v[:, k : k + 128] for k in range(0, strip_c, 128))
        sums_ref[0] += lanes(grads)
        sums_ref[1] += lanes(pens)


def make_grad(rows_all, delta_all, rounding, scale_row):
    tokens, rows = rows_all.shape
    cols = delta_all.shape[1]
    tr, tc = tile_of(rows, 256), tile_of(cols, 2048)
    return pl.pallas_call(
        grad_kernel,
        out_shape=(
            jax.ShapeDtypeStruct((rows, cols), jnp.bfloat16),
            jax.ShapeDtypeStruct((2, 8, 128), jnp.float32),
        ),
        grid=(cols // tc, rows // tr),
        in_specs=[
            pl.BlockSpec((tokens, tr), lambda j, i: (0, i)),
            pl.BlockSpec((tokens, tc), lambda j, i: (0, j)),
            pl.BlockSpec((tr, tc), lambda j, i: (i, j)),
            pl.BlockSpec((1, tc), lambda j, i: (0, j)),
        ],
        out_specs=(
            pl.BlockSpec((tr, tc), lambda j, i: (i, j)),
            pl.BlockSpec((2, 8, 128), lambda j, i: (0, 0, 0)),
        ),
        scratch_shapes=[pltpu.VMEM((tr, tc), jnp.float32)],
        compiler_params=pltpu.CompilerParams(dimension_semantics=("arbitrary", "arbitrary")),
        cost_estimate=pl.CostEstimate(
            flops=2 * tokens * rows * cols, transcendentals=rows * cols, bytes_accessed=6 * rows * cols
        ),
    )(rows_all, delta_all, rounding, scale_row)


def chain_kernel(
    act_ref, target_ref, weight_hbm, gain_ref, gain_next_ref,
    out_ref, residue_ref, rows_hbm, delta_hbm,
    weight, rows, part, own, landed, joined, carried, normed, normed0, stat, delta,
    w_sem, row_sem, relay_sem, mate_send, join_send, join_recv, land_send, land_recv, carry_sem, carry_recv,
    norm_send, norm0_send, stat_send, stat_recv, delta_send, delta_recv, store_sem,
):
    section, z, t = (lax.axis_index(name) for name in ("section", "dp", "tensor"))
    sections, dp, nt = (lax.axis_size(name) for name in ("section", "dp", "tensor"))
    micro, _, tok, depth = rows.shape
    cols = out_ref.shape[1]
    pieces = cols // depth
    wide = cols // SPLIT
    model = depth * dp
    first = section == 0
    inner = section < sections - 1

    def remote(src, dst, send, recv, s, d, c):
        return pltpu.make_async_remote_copy(
            src_ref=src, dst_ref=dst, send_sem=send, recv_sem=recv,
            device_id={"section": s, "dp": d, "tensor": c}, device_id_type=pl.DeviceIdType.MESH,
        )

    def arrived(dst, recv):
        remote(dst, dst, recv, recv, section, z, t).wait_recv()

    def left(src, send):
        remote(src, src, send, send, section, z, t).wait_send()

    def columns(q):
        return pl.ds(q * wide, wide)

    def weight_copy(q):
        return pltpu.make_async_copy(
            weight_hbm.at[:, columns(q)], weight.at[:, columns(q)], w_sem.at[q]
        )

    for q in range(SPLIT):
        weight_copy(q).start()

    def token_rows(m):
        return pl.ds(m * tok, tok)

    def stat_start(kind, m, total):
        stat[kind, m, t] = jnp.broadcast_to(total, (tok, 128))
        for k in range(1, nt):
            remote(
                stat.at[kind, m, t], stat.at[kind, m, t], stat_send.at[kind, m, k], stat_recv.at[kind, m, t],
                section, z, lax.rem(t + k, nt),
            ).start()

    def inverse(kind, m):
        for k in range(1, nt):
            other = lax.rem(t + k, nt)
            arrived(stat.at[kind, m, other], stat_recv.at[kind, m, other])
        total = stat[kind, m, 0][:, :1]
        for k in range(1, nt):
            total = total + stat[kind, m, k][:, :1]
        return lax.rsqrt(total / model + norm_eps)

    entry = lax.rem(z, nt)

    def at_home(c):
        return first & (t * pieces + c == z) & (entry == t)

    def norm_copy(m, c, initial):
        buf, sem = (normed0, norm0_send) if initial else (normed, norm_send)
        return remote(
            buf.at[m, c], rows.at[m, z], sem.at[m, c], row_sem.at[m, z],
            section if initial else section + 1, t * pieces + c, entry,
        )

    def spread(m, src, gain, initial):
        inv = inverse(0 if initial else 1, m)
        buf = normed0 if initial else normed
        for c in range(pieces):
            cut = pl.ds(c * depth, depth)
            value = (src[token_rows(m), cut].astype(jnp.float32) * inv * gain[:, cut]).astype(jnp.bfloat16)
            buf[m, c] = value
            if initial:

                @pl.when(at_home(c))
                def _():
                    rows[m, z] = value

                @pl.when(jnp.logical_not(at_home(c)))
                def _():
                    norm_copy(m, c, True).start()
            else:
                norm_copy(m, c, False).start()

    @pl.when(first)
    def _():
        for m in range(micro):
            value = act_ref[token_rows(m), :]
            carried[m] = value
            value = value.astype(jnp.float32)
            stat_start(0, m, jnp.sum(value * value, axis=1, keepdims=True))
        for m in range(micro):
            spread(m, act_ref, gain_ref, True)

    home_piece = lax.rem(z, pieces)
    is_sender = t == z // pieces

    def relay(m, o, k):
        return remote(
            rows.at[m, o], rows.at[m, o], relay_sem.at[m, o, k], row_sem.at[m, o],
            section, z, lax.rem(t + k, nt),
        )

    def receive_rows(m):
        for o in range(dp):
            local = first & (z == o) & is_sender

            @pl.when((t == o % nt) & jnp.logical_not(local))
            def _():
                arrived(rows.at[m, o], row_sem.at[m, o])

            @pl.when(t == o % nt)
            def _():
                for k in range(1, nt):
                    relay(m, o, k).start()

        for o in range(dp):

            @pl.when(t != o % nt)
            def _():
                arrived(rows.at[m, o], row_sem.at[m, o])

    def rows_store(m):
        return pltpu.make_async_copy(rows.at[m], rows_hbm.at[m], store_sem.at[m])

    side = dp // 2
    place = lax.rem(z, side)
    across = (1 - z // side) * side
    is_inner = place == (side - 1) * (1 - z // side)
    inner_here = jnp.where(z < side, side - 1, side)

    def mate_copy(m, k):
        mate = z - place + lax.rem(place + k, side)
        return remote(
            part.at[m, mate], landed.at[m, place], mate_send.at[m, k], land_recv.at[m, 0, place], section, mate, t
        )

    def join_copy(m, q, o):
        return remote(
            part.at[m, across + o, :, columns(q)], joined.at[m, place, o, :, columns(q)],
            join_send.at[m, q, o], join_recv.at[m, q, place, o], section, inner_here, t,
        )

    def land_copy(m, q, o):
        return remote(
            part.at[m, across + o, :, columns(q)], landed.at[m, o, :, columns(q)],
            land_send.at[m, q, o], land_recv.at[m, q, o], section, across + o, t,
        )

    def multiply(m):
        step = tile_of(wide, 256)
        for q in range(SPLIT):
            if m == 0:
                weight_copy(q).wait()

            @pl.loop(0, wide // step)
            def _(b):
                cut = pl.ds(pl.multiple_of(q * wide + b * step, step), step)
                value = jnp.dot(
                    rows[m].reshape(dp * tok, depth), weight[:, cut], preferred_element_type=jnp.float32
                )
                own[m % 2, :, :, cut] = value.reshape(dp, tok, step)
                part[m, :, :, cut] = value.reshape(dp, tok, step).astype(jnp.bfloat16)

            @pl.when(jnp.logical_not(is_inner))
            def _():
                for o in range(side):
                    join_copy(m, q, o).start()

        for k in range(1, side):
            mate_copy(m, k).start()

    def combine(m):
        @pl.when(is_inner)
        def _():
            for q in range(SPLIT):
                for o in range(side):
                    total = own[m % 2, across + o, :, columns(q)]
                    for k in range(1, side):
                        mate = lax.rem(place + k, side)
                        arrived(joined.at[m, mate, o, :, columns(q)], join_recv.at[m, q, mate, o])
                        total = total + joined[m, mate, o, :, columns(q)].astype(jnp.float32)
                    part[m, across + o, :, columns(q)] = total.astype(jnp.bfloat16)
                    land_copy(m, q, o).start()

    def hand_on(m, origin, way):
        return remote(
            delta.at[m, origin], delta.at[m, origin], delta_send.at[m, origin, way], delta_recv.at[m, origin],
            section, z + (1 if way else -1), t,
        )

    def gather_step(m, hop):
        for way in (0, 1):
            origin = z - hop if way else z + hop
            exists = (origin >= 0) & (origin < dp)
            onward = exists & ((z + 1 < dp) if way else (z >= 1))
            if hop:

                @pl.when(exists)
                def _():
                    arrived(delta.at[m, origin], delta_recv.at[m, origin])

            @pl.when(onward)
            def _():
                hand_on(m, origin, way).start()

    def finish(m):
        total = jnp.zeros((tok, 1), jnp.float32)
        squares = jnp.zeros((tok, 1), jnp.float32)

        @pl.when(jnp.logical_not(first))
        def _():
            arrived(carried.at[m], carry_recv.at[m])

        for q in range(SPLIT):
            arrived(landed.at[m, place, :, columns(q)], land_recv.at[m, q, place])
            if q == 0:
                for k in range(1, side):
                    mate = lax.rem(place + k, side)
                    arrived(landed.at[m, mate], land_recv.at[m, 0, mate])
            branch = own[m % 2, z, :, columns(q)]
            for k in range(side):
                branch = branch + landed[m, lax.rem(place + k, side), :, columns(q)].astype(jnp.float32)
            value = (carried[m, :, columns(q)].astype(jnp.float32) + branch).astype(jnp.bfloat16)
            out_ref[token_rows(m), columns(q)] = value
            value = value.astype(jnp.float32)
            residue = value - target_ref[token_rows(m), columns(q)].astype(jnp.float32)
            delta[m, z, :, columns(q)] = (error_scale / (micro * dp * tok) ** 0.5 * residue).astype(jnp.bfloat16)
            total = total + jnp.sum(value * value, axis=1, keepdims=True)
            squares = squares + jnp.sum(residue * residue, axis=1, keepdims=True)
        residue_ref[token_rows(m), :] = jnp.broadcast_to(squares, (tok, 128))

        @pl.when(inner)
        def _():
            stat_start(1, m, total)
            carry_copy(m).start()
            spread(m, out_ref, gain_next_ref, False)

    def carry_copy(m):
        return remote(
            out_ref.at[token_rows(m), :], carried.at[m], carry_sem.at[m], carry_recv.at[m], section + 1, z, t
        )

    def complete(m):
        finish(m)
        for hop in range(min(dp, m + 1)):
            gather_step(m - hop, hop)

    for m in range(micro):
        receive_rows(m)
        rows_store(m).start()
        multiply(m)
        if m:
            complete(m - 1)
        combine(m)
    complete(micro - 1)
    for late in range(micro, micro + dp - 1):
        for hop in range(dp):
            if 0 <= late - hop < micro:
                gather_step(late - hop, hop)
    delta_store = pltpu.make_async_copy(delta, delta_hbm, store_sem.at[micro])
    delta_store.start()

    for m in range(micro):
        for k in range(1, side):
            mate_copy(m, k).wait_send()
        for q in range(SPLIT):
            for o in range(side):

                @pl.when(is_inner)
                def _():
                    land_copy(m, q, o).wait_send()

                @pl.when(jnp.logical_not(is_inner))
                def _():
                    join_copy(m, q, o).wait_send()

        for o in range(dp):

            @pl.when(t == o % nt)
            def _():
                for k in range(1, nt):
                    relay(m, o, k).wait_send()

            for way in (0, 1):
                onward = ((z + 1 < dp) & (o <= z)) if way else ((z >= 1) & (o >= z))

                @pl.when(onward)
                def _():
                    hand_on(m, o, way).wait_send()

        @pl.when(first)
        def _():
            for k in range(1, nt):
                left(stat.at[0, m, t], stat_send.at[0, m, k])
            for c in range(pieces):

                @pl.when(jnp.logical_not(at_home(c)))
                def _():
                    norm_copy(m, c, True).wait_send()

        @pl.when(inner)
        def _():
            for k in range(1, nt):
                left(stat.at[1, m, t], stat_send.at[1, m, k])
            carry_copy(m).wait_send()
            for c in range(pieces):
                norm_copy(m, c, False).wait_send()

        rows_store(m).wait()
    delta_store.wait()


def run_chain(activations, targets, weight, gain_row, gain_next, dp, nt):
    tok_dev, cols = activations.shape
    depth = weight.shape[0]
    tok = tok_dev // MICRO
    pieces = cols // depth
    side = dp // 2
    bf16, f32 = jnp.bfloat16, jnp.float32
    vmem = pl.BlockSpec(memory_space=pltpu.VMEM)
    hbm = pl.BlockSpec(memory_space=pl.ANY)
    dma = pltpu.SemaphoreType.DMA
    out, residue, rows_all, delta_all = pl.pallas_call(
        chain_kernel,
        out_shape=(
            jax.ShapeDtypeStruct((tok_dev, cols), bf16),
            jax.ShapeDtypeStruct((tok_dev, 128), f32),
            jax.ShapeDtypeStruct((MICRO, dp, tok, depth), bf16),
            jax.ShapeDtypeStruct((MICRO, dp, tok, cols), bf16),
        ),
        in_specs=[vmem, vmem, hbm, vmem, vmem],
        out_specs=(vmem, vmem, hbm, hbm),
        scratch_shapes=[
            pltpu.VMEM((depth, cols), bf16),
            pltpu.VMEM((MICRO, dp, tok, depth), bf16),
            pltpu.VMEM((MICRO, dp, tok, cols), bf16),
            pltpu.VMEM((2, dp, tok, cols), f32),
            pltpu.VMEM((MICRO, side, tok, cols), bf16),
            pltpu.VMEM((MICRO, side, side, tok, cols), bf16),
            pltpu.VMEM((MICRO, tok, cols), bf16),
            pltpu.VMEM((MICRO, pieces, tok, depth), bf16),
            pltpu.VMEM((MICRO, pieces, tok, depth), bf16),
            pltpu.VMEM((2, MICRO, nt, tok, 128), f32),
            pltpu.VMEM((MICRO, dp, tok, cols), bf16),
            dma((SPLIT,)),
            dma((MICRO, dp)),
            dma((MICRO, dp, nt)),
            dma((MICRO, side)),
            dma((MICRO, SPLIT, side)),
            dma((MICRO, SPLIT, side, side)),
            dma((MICRO, SPLIT, side)),
            dma((MICRO, SPLIT, side)),
            dma((MICRO,)),
            dma((MICRO,)),
            dma((MICRO, pieces)),
            dma((MICRO, pieces)),
            dma((2, MICRO, nt)),
            dma((2, MICRO, nt)),
            dma((MICRO, dp, 2)),
            dma((MICRO, dp)),
            dma((MICRO + 1,)),
        ],
        compiler_params=pltpu.CompilerParams(has_side_effects=True, vmem_limit_bytes=VMEM_ALL),
        cost_estimate=pl.CostEstimate(
            flops=2 * tok_dev * dp * depth * cols, transcendentals=0, bytes_accessed=2 * depth * cols
        ),
    )(activations, targets, weight, gain_row, gain_next)
    return out, residue, rows_all.reshape(-1, depth), delta_all.reshape(-1, cols)


def sums_kernel(mine_ref, total_ref, held, send_sem, recv_sem):
    z, t = lax.axis_index("dp"), lax.axis_index("tensor")
    dp, nt = lax.axis_size("dp"), lax.axis_size("tensor")
    place = z * nt + t
    count = dp * nt

    def copy(k):
        peer = lax.rem(place + k, count)
        return pltpu.make_async_remote_copy(
            src_ref=mine_ref, dst_ref=held.at[place], send_sem=send_sem.at[k], recv_sem=recv_sem.at[place],
            device_id={"dp": peer // nt, "tensor": lax.rem(peer, nt)}, device_id_type=pl.DeviceIdType.MESH,
        )

    for k in range(1, count):
        copy(k).start()
    held[place] = mine_ref[...]
    for k in range(1, count):
        peer = lax.rem(place + k, count)
        pltpu.make_async_remote_copy(
            src_ref=mine_ref, dst_ref=held.at[peer], send_sem=send_sem.at[k], recv_sem=recv_sem.at[peer],
            device_id={"dp": z, "tensor": t}, device_id_type=pl.DeviceIdType.MESH,
        ).wait_recv()
    total = held[0]
    for k in range(1, count):
        total = total + held[k]
    total = jnp.sum(total, axis=1, keepdims=True)
    total_ref[...] = jnp.broadcast_to(jnp.sum(total, axis=2, keepdims=True), total_ref.shape)
    for k in range(1, count):
        copy(k).wait_send()


def add_sums(mine, count):
    vmem = pl.BlockSpec(memory_space=pltpu.VMEM)
    return pl.pallas_call(
        sums_kernel,
        out_shape=jax.ShapeDtypeStruct(mine.shape, mine.dtype),
        in_specs=[vmem],
        out_specs=vmem,
        scratch_shapes=[
            pltpu.VMEM((count,) + mine.shape, mine.dtype),
            pltpu.SemaphoreType.DMA((count,)),
            pltpu.SemaphoreType.DMA((count,)),
        ],
        compiler_params=pltpu.CompilerParams(has_side_effects=True),
    )(mine)[:, 0, 0]


def passed_along(value, axis, steps):
    count = lax.axis_size(axis)
    leading, last = (max(0, -steps), min(count, count - steps))
    return lax.ppermute(value, axis, [(source, source + steps) for source in range(leading, last)])


def normalize(features, gain_row):
    inputs = features.astype(jnp.float32)
    mean_sq = jnp.mean(inputs * inputs, axis=1, keepdims=True)
    return (inputs * lax.rsqrt(mean_sq + norm_eps) * gain_row[None, :]).astype(jnp.bfloat16)


def ticked_chain(activations, targets, weight, gain_row):
    section_index = lax.axis_index("section")
    section_count = lax.axis_size("section")
    dp_count = lax.axis_size("dp")
    tok_dev, width_local = activations.shape
    token_total = tok_dev * dp_count
    tok_micro = tok_dev // TICKS
    received = jnp.zeros((tok_micro, width_local), jnp.bfloat16)
    row_ticks = []
    output_ticks = []
    tick_count = TICKS + section_count - 1
    for tick_index in range(tick_count):
        fed = min(tick_index, TICKS - 1) * tok_micro
        block_input = jnp.where(section_index == 0, activations[fed : fed + tok_micro], received)
        whole_rows = lax.all_gather(block_input, "tensor", axis=1, tiled=True)
        normed = normalize(whole_rows, gain_row)
        swapped = lax.all_to_all(normed, "dp", split_axis=1, concat_axis=0, tiled=True)
        partial_value = jnp.dot(swapped, weight, preferred_element_type=jnp.float32)
        branch = lax.psum_scatter(partial_value, "dp", scatter_dimension=0, tiled=True)
        block_result = (block_input.astype(jnp.float32) + branch).astype(jnp.bfloat16)
        row_ticks.append(swapped)
        output_ticks.append(block_result)
        if tick_index + 1 < tick_count:
            received = passed_along(block_result, "section", 1)
    stored_rows = lax.dynamic_slice_in_dim(jnp.stack(row_ticks), section_index, TICKS, axis=0)
    stored_rows = stored_rows.reshape(TICKS, dp_count, tok_micro, -1).transpose(1, 0, 2, 3)
    outputs_buf = lax.dynamic_slice_in_dim(
        jnp.concatenate(output_ticks), section_index * tok_micro, tok_dev, axis=0
    )
    residue = outputs_buf.astype(jnp.float32) - targets.astype(jnp.float32)
    delta = (error_scale / token_total**0.5 * residue).astype(jnp.bfloat16)
    delta_all = lax.all_gather(delta, "dp", axis=0, tiled=True)
    rows_all = stored_rows.reshape(dp_count * tok_dev, -1)
    return outputs_buf, jnp.sum(residue * residue, axis=1), rows_all, delta_all


def per_device(activations, targets, packed_floors, rounding, scales, norm_gains):
    dp_count = lax.axis_size("dp")
    core_count = lax.axis_size("tensor")
    tok_dev, width_local = activations.shape
    width_full = norm_gains.shape[1]
    token_total = tok_dev * dp_count
    weight = make_weight(packed_floors[0], rounding[0], scales)
    chained = width_local % rounding.shape[1] == 0 and dp_count % core_count == 0 and dp_count % 2 == 0
    if chained:
        here = lax.axis_index("tensor") * width_local
        gain_row = lax.dynamic_slice_in_dim(norm_gains, here, width_local, axis=1)
        gain_next = passed_along(gain_row, "section", -1)
        outputs_buf, residues, rows_all, delta_all = run_chain(
            activations, targets[0], weight, gain_row, gain_next, dp_count, core_count
        )
    else:
        outputs_buf, residues, rows_all, delta_all = ticked_chain(
            activations, targets[0], weight, norm_gains[0]
        )
    grad, sums = make_grad(rows_all, delta_all, rounding[0], scales)
    if chained:
        recon = jnp.where(lax.broadcasted_iota(jnp.int32, residues.shape, 1) == 0, residues, 0.0)
        recon = recon.reshape(-1, 8, 128).sum(axis=0)
        square_sum, penalty_sum, recon_sum = add_sums(
            jnp.concatenate([sums, recon[None]]), dp_count * core_count
        )
    else:
        recon_sum, penalty_sum, square_sum = lax.psum(
            (jnp.sum(residues), jnp.sum(sums[1]), jnp.sum(sums[0])), ("dp", "tensor")
        )
    mean_grad = square_sum / (width_full * width_full) + grad_eps
    rounding_next = rounding[0] - step_rate * grad.astype(jnp.float32) * lax.rsqrt(mean_grad)
    loss_value = recon_sum / (token_total * width_full) + reg_weight * penalty_sum / (
        width_full * width_full
    )
    return (rounding_next[None], outputs_buf[None], loss_value.reshape(1))


def solution(mesh):
    placed = (
        P("dp", "tensor"),
        P("section", "dp", "tensor"),
        P("section", "dp", "tensor"),
        P("section", "dp", "tensor"),
        P("section", "tensor"),
        P("section", None),
    )
    return jax.shard_map(
        per_device,
        mesh=mesh,
        in_specs=placed,
        out_specs=(P("section", "dp", "tensor"), P("section", "dp", "tensor"), P("section")),
        check_vma=False,
    )
```

```python
import functools
import jax
import jax.numpy as jnp
from jax import lax
from jax.experimental import pallas as pl
from jax.experimental.pallas import tpu as pltpu
from jax.sharding import PartitionSpec as P

MICRO = 8
TICKS = 4
SPLIT = 4
LAG = 2


norm_eps = 1e-06
grad_eps = 1e-06
reg_weight = 0.3
step_rate = 0.25
error_scale = 600.0

VMEM_ALL = 62 * 1024 * 1024


def tile_of(size, most):
    while size % most:
        most //= 2
    return most


def weight_kernel(packed_ref, rounding_ref, scale_ref, weight_ref):
    rows, cols = rounding_ref.shape
    strip_c = tile_of(cols, 1024)
    strip_r = 32

    @pl.loop(0, cols // strip_c)
    def _(cb):
        col = pl.ds(pl.multiple_of(cb * strip_c, strip_c), strip_c)
        scale = scale_ref[:, col]
        place = lax.broadcasted_iota(jnp.int32, (8, strip_c), 0)
        shift = 3 * (place & 3)
        upper = place < 4

        @pl.loop(0, rows // strip_r)
        def _(rb):
            values = []
            for k in range(strip_r // 8):
                row = pl.ds(pl.multiple_of(rb * strip_r, strip_r) + 8 * k, 8)
                first = packed_ref[pl.ds(rb * (strip_r // 4) + 2 * k, 1), col]
                second = packed_ref[pl.ds(rb * (strip_r // 4) + 2 * k + 1, 1), col]
                words = jnp.where(
                    upper, jnp.broadcast_to(first, upper.shape), jnp.broadcast_to(second, upper.shape)
                )
                codes = (jnp.right_shift(words, shift) & 7).astype(jnp.float32)
                part = jnp.clip(0.6 * jnp.tanh(0.5 * rounding_ref[row, col]) - 3.5, -4.0, -3.0)
                values.append(scale * (codes + part))
            row = pl.ds(pl.multiple_of(rb * strip_r, strip_r), strip_r)
            weight_ref[row, col] = jnp.concatenate(values, axis=0).astype(jnp.bfloat16)


def make_weight(packed, rounding, scale_row):
    rows, cols = rounding.shape
    tr, tc = tile_of(rows, 256), tile_of(cols, 2048)
    return pl.pallas_call(
        weight_kernel,
        out_shape=jax.ShapeDtypeStruct((rows, cols), jnp.bfloat16),
        grid=(cols // tc, rows // tr),
        in_specs=[
            pl.BlockSpec((tr // 4, tc), lambda j, i: (i, j)),
            pl.BlockSpec((tr, tc), lambda j, i: (i, j)),
            pl.BlockSpec((1, tc), lambda j, i: (0, j)),
        ],
        out_specs=pl.BlockSpec((tr, tc), lambda j, i: (i, j)),
        compiler_params=pltpu.CompilerParams(dimension_semantics=("arbitrary", "arbitrary")),
        cost_estimate=pl.CostEstimate(
            flops=20 * rows * cols, transcendentals=rows * cols, bytes_accessed=7 * rows * cols
        ),
    )(packed, rounding, scale_row)


def grad_kernel(rows_ref, delta_ref, rounding_ref, scale_ref, grad_ref, sums_ref, product):
    trow, tcol = rounding_ref.shape
    strip_c = tile_of(tcol, 512)
    strip_r = 64
    first = (pl.program_id(0) == 0) & (pl.program_id(1) == 0)

    @pl.when(first)
    def _():
        sums_ref[...] = jnp.zeros_like(sums_ref)

    product[...] = lax.dot_general(
        rows_ref[...], delta_ref[...], (((0,), (0,)), ((), ())), preferred_element_type=jnp.float32
    )

    @pl.loop(0, tcol // strip_c)
    def _(cb):
        col = pl.ds(pl.multiple_of(cb * strip_c, strip_c), strip_c)
        scale = (0.3 / 1.44 / 4.0) * scale_ref[:, col]

        def strip(rb, sums):
            row = pl.ds(pl.multiple_of(rb * strip_r, strip_r), strip_r)
            half = jnp.clip(0.6 * jnp.tanh(0.5 * rounding_ref[row, col]), -0.5, 0.5)
            square = half * half
            slope = jnp.where(square < 0.25, 0.36 - square, 0.0)
            grad = slope * (scale * product[row, col] - square * half)
            grad_ref[row, col] = grad.astype(grad_ref.dtype)
            fold = lambda v: v.reshape(strip_r // 8, 8, strip_c).sum(axis=0)
            return sums[0] + fold(grad * grad), sums[1] + fold(0.0625 - square * square)

        zero = jnp.zeros((8, strip_c), jnp.float32)
        grads, pens = lax.fori_loop(0, trow // strip_r, strip, (zero, zero))
        lanes = lambda v: sum(v[:, k : k + 128] for k in range(0, strip_c, 128))
        sums_ref[0] += lanes(grads)
        sums_ref[1] += lanes(pens)


def make_grad(rows_all, delta_all, rounding, scale_row):
    tokens, rows = rows_all.shape
    cols = delta_all.shape[1]
    tr, tc = tile_of(rows, 256), tile_of(cols, 2048)
    return pl.pallas_call(
        grad_kernel,
        out_shape=(
            jax.ShapeDtypeStruct((rows, cols), jnp.bfloat16),
            jax.ShapeDtypeStruct((2, 8, 128), jnp.float32),
        ),
        grid=(cols // tc, rows // tr),
        in_specs=[
            pl.BlockSpec((tokens, tr), lambda j, i: (0, i)),
            pl.BlockSpec((tokens, tc), lambda j, i: (0, j)),
            pl.BlockSpec((tr, tc), lambda j, i: (i, j)),
            pl.BlockSpec((1, tc), lambda j, i: (0, j)),
        ],
        out_specs=(
            pl.BlockSpec((tr, tc), lambda j, i: (i, j)),
            pl.BlockSpec((2, 8, 128), lambda j, i: (0, 0, 0)),
        ),
        scratch_shapes=[pltpu.VMEM((tr, tc), jnp.float32)],
        compiler_params=pltpu.CompilerParams(dimension_semantics=("arbitrary", "arbitrary")),
        cost_estimate=pl.CostEstimate(
            flops=2 * tokens * rows * cols, transcendentals=rows * cols, bytes_accessed=6 * rows * cols
        ),
    )(rows_all, delta_all, rounding, scale_row)


def chain_kernel(
    act_ref, target_ref, weight_hbm, gain_ref, gain_next_ref,
    out_ref, residue_ref, rows_hbm, delta_hbm,
    weight, rows, part, own, landed, joined, carried, normed, normed0, stat, delta,
    w_sem, row_sem, relay_sem, mate_send, join_send, join_recv, land_send, land_recv, carry_sem, carry_recv,
    norm_send, norm0_send, stat_send, stat_recv, delta_send, delta_recv, store_sem,
):
    section, z, t = (lax.axis_index(name) for name in ("section", "dp", "tensor"))
    sections, dp, nt = (lax.axis_size(name) for name in ("section", "dp", "tensor"))
    micro, _, tok, depth = rows.shape
    cols = out_ref.shape[1]
    pieces = cols // depth
    wide = cols // SPLIT
    model = depth * dp
    first = section == 0
    inner = section < sections - 1

    def remote(src, dst, send, recv, s, d, c):
        return pltpu.make_async_remote_copy(
            src_ref=src, dst_ref=dst, send_sem=send, recv_sem=recv,
            device_id={"section": s, "dp": d, "tensor": c}, device_id_type=pl.DeviceIdType.MESH,
        )

    def arrived(dst, recv):
        remote(dst, dst, recv, recv, section, z, t).wait_recv()

    def left(src, send):
        remote(src, src, send, send, section, z, t).wait_send()

    def columns(q):
        return pl.ds(q * wide, wide)

    def weight_copy(q):
        return pltpu.make_async_copy(
            weight_hbm.at[:, columns(q)], weight.at[:, columns(q)], w_sem.at[q]
        )

    for q in range(SPLIT):
        weight_copy(q).start()

    def token_rows(m):
        return pl.ds(m * tok, tok)

    def stat_start(kind, m, total):
        stat[kind, m, t] = jnp.broadcast_to(total, (tok, 128))
        for k in range(1, nt):
            remote(
                stat.at[kind, m, t], stat.at[kind, m, t], stat_send.at[kind, m, k], stat_recv.at[kind, m, t],
                section, z, lax.rem(t + k, nt),
            ).start()

    def inverse(kind, m):
        for k in range(1, nt):
            other = lax.rem(t + k, nt)
            arrived(stat.at[kind, m, other], stat_recv.at[kind, m, other])
        total = stat[kind, m, 0][:, :1]
        for k in range(1, nt):
            total = total + stat[kind, m, k][:, :1]
        return lax.rsqrt(total / model + norm_eps)

    entry = lax.rem(z, nt)

    def at_home(c):
        return first & (t * pieces + c == z) & (entry == t)

    def norm_copy(m, c, initial):
        buf, sem = (normed0, norm0_send) if initial else (normed, norm_send)
        return remote(
            buf.at[m, c], rows.at[m, z], sem.at[m, c], row_sem.at[m, z],
            section if initial else section + 1, t * pieces + c, entry,
        )

    def spread(m, src, gain, initial):
        inv = inverse(0 if initial else 1, m)
        buf = normed0 if initial else normed
        for c in range(pieces):
            cut = pl.ds(c * depth, depth)
            value = (src[token_rows(m), cut].astype(jnp.float32) * inv * gain[:, cut]).astype(jnp.bfloat16)
            buf[m, c] = value
            if initial:

                @pl.when(at_home(c))
                def _():
                    rows[m, z] = value

                @pl.when(jnp.logical_not(at_home(c)))
                def _():
                    norm_copy(m, c, True).start()
            else:
                norm_copy(m, c, False).start()

    @pl.when(first)
    def _():
        for m in range(micro):
            value = act_ref[token_rows(m), :]
            carried[m] = value
            value = value.astype(jnp.float32)
            stat_start(0, m, jnp.sum(value * value, axis=1, keepdims=True))
        for m in range(micro):
            spread(m, act_ref, gain_ref, True)

    home_piece = lax.rem(z, pieces)
    is_sender = t == z // pieces

    def relay(m, o, k):
        return remote(
            rows.at[m, o], rows.at[m, o], relay_sem.at[m, o, k], row_sem.at[m, o],
            section, z, lax.rem(t + k, nt),
        )

    def receive_rows(m):
        for o in range(dp):
            local = first & (z == o) & is_sender

            @pl.when((t == o % nt) & jnp.logical_not(local))
            def _():
                arrived(rows.at[m, o], row_sem.at[m, o])

            @pl.when(t == o % nt)
            def _():
                for k in range(1, nt):
                    relay(m, o, k).start()

        for o in range(dp):

            @pl.when(t != o % nt)
            def _():
                arrived(rows.at[m, o], row_sem.at[m, o])

    def rows_store(m):
        return pltpu.make_async_copy(rows.at[m], rows_hbm.at[m], store_sem.at[m])

    side = dp // 2
    place = lax.rem(z, side)
    across = (1 - z // side) * side
    is_inner = place == (side - 1) * (1 - z // side)
    inner_here = jnp.where(z < side, side - 1, side)

    def mate_copy(m, k):
        mate = z - place + lax.rem(place + k, side)
        return remote(
            part.at[m, mate], landed.at[m, place], mate_send.at[m, k], land_recv.at[m, 0, place], section, mate, t
        )

    def join_copy(m, q, o):
        return remote(
            part.at[m, across + o, :, columns(q)], joined.at[m, place, o, :, columns(q)],
            join_send.at[m, q, o], join_recv.at[m, q, place, o], section, inner_here, t,
        )

    def land_copy(m, q, o):
        return remote(
            part.at[m, across + o, :, columns(q)], landed.at[m, o, :, columns(q)],
            land_send.at[m, q, o], land_recv.at[m, q, o], section, across + o, t,
        )

    def multiply(m):
        step = tile_of(wide, 256)
        for q in range(SPLIT):
            if m == 0:
                weight_copy(q).wait()

            @pl.loop(0, wide // step)
            def _(b):
                cut = pl.ds(pl.multiple_of(q * wide + b * step, step), step)
                value = jnp.dot(
                    rows[m].reshape(dp * tok, depth), weight[:, cut], preferred_element_type=jnp.float32
                )
                own[m % 2, :, :, cut] = value.reshape(dp, tok, step)
                part[m, :, :, cut] = value.reshape(dp, tok, step).astype(jnp.bfloat16)

            @pl.when(jnp.logical_not(is_inner))
            def _():
                for o in range(side):
                    join_copy(m, q, o).start()

        for k in range(1, side):
            mate_copy(m, k).start()

    def combine(m):
        @pl.when(is_inner)
        def _():
            for q in range(SPLIT):
                for o in range(side):
                    total = own[m % 2, across + o, :, columns(q)]
                    for k in range(1, side):
                        mate = lax.rem(place + k, side)
                        arrived(joined.at[m, mate, o, :, columns(q)], join_recv.at[m, q, mate, o])
                        total = total + joined[m, mate, o, :, columns(q)].astype(jnp.float32)
                    part[m, across + o, :, columns(q)] = total.astype(jnp.bfloat16)
                    land_copy(m, q, o).start()

    def hand_on(m, origin, way):
        return remote(
            delta.at[m, origin], delta.at[m, origin], delta_send.at[m, origin, way], delta_recv.at[m, origin],
            section, z + (1 if way else -1), t,
        )

    def gather_step(m, hop):
        for way in (0, 1):
            origin = z - hop if way else z + hop
            exists = (origin >= 0) & (origin < dp)
            onward = exists & ((z + 1 < dp) if way else (z >= 1))
            if hop:

                @pl.when(exists)
                def _():
                    arrived(delta.at[m, origin], delta_recv.at[m, origin])

            @pl.when(onward)
            def _():
                hand_on(m, origin, way).start()

    def finish(m):
        total = jnp.zeros((tok, 1), jnp.float32)
        squares = jnp.zeros((tok, 1), jnp.float32)

        @pl.when(jnp.logical_not(first))
        def _():
            arrived(carried.at[m], carry_recv.at[m])

        for q in range(SPLIT):
            arrived(landed.at[m, place, :, columns(q)], land_recv.at[m, q, place])
            if q == 0:
                for k in range(1, side):
                    mate = lax.rem(place + k, side)
                    arrived(landed.at[m, mate], land_recv.at[m, 0, mate])
            branch = own[m % 2, z, :, columns(q)]
            for k in range(side):
                branch = branch + landed[m, lax.rem(place + k, side), :, columns(q)].astype(jnp.float32)
            value = (carried[m, :, columns(q)].astype(jnp.float32) + branch).astype(jnp.bfloat16)
            out_ref[token_rows(m), columns(q)] = value
            value = value.astype(jnp.float32)
            residue = value - target_ref[token_rows(m), columns(q)].astype(jnp.float32)
            delta[m, z, :, columns(q)] = (error_scale / (micro * dp * tok) ** 0.5 * residue).astype(jnp.bfloat16)
            total = total + jnp.sum(value * value, axis=1, keepdims=True)
            squares = squares + jnp.sum(residue * residue, axis=1, keepdims=True)
        residue_ref[token_rows(m), :] = jnp.broadcast_to(squares, (tok, 128))

        @pl.when(inner)
        def _():
            stat_start(1, m, total)
            carry_copy(m).start()
            spread(m, out_ref, gain_next_ref, False)

    def carry_copy(m):
        return remote(
            out_ref.at[token_rows(m), :], carried.at[m], carry_sem.at[m], carry_recv.at[m], section + 1, z, t
        )

    eager = section >= sections - 2

    def gather(now):
        for hop in range(dp):
            if 0 <= now - LAG * hop < micro:
                gather_step(now - LAG * hop, hop)

    for m in range(micro + 1):
        if m < micro:
            receive_rows(m)
            rows_store(m).start()
            multiply(m)
        if m:
            finish(m - 1)
        if m < micro:
            combine(m)
        if m:

            @pl.when(eager)
            def _():
                gather(m - 1)

    @pl.when(jnp.logical_not(eager))
    def _():
        for now in range(micro):
            gather(now)

    for now in range(micro, micro + LAG * (dp - 1)):
        gather(now)
    delta_store = pltpu.make_async_copy(delta, delta_hbm, store_sem.at[micro])
    delta_store.start()

    for m in range(micro):
        for k in range(1, side):
            mate_copy(m, k).wait_send()
        for q in range(SPLIT):
            for o in range(side):

                @pl.when(is_inner)
                def _():
                    land_copy(m, q, o).wait_send()

                @pl.when(jnp.logical_not(is_inner))
                def _():
                    join_copy(m, q, o).wait_send()

        for o in range(dp):

            @pl.when(t == o % nt)
            def _():
                for k in range(1, nt):
                    relay(m, o, k).wait_send()

            for way in (0, 1):
                onward = ((z + 1 < dp) & (o <= z)) if way else ((z >= 1) & (o >= z))

                @pl.when(onward)
                def _():
                    hand_on(m, o, way).wait_send()

        @pl.when(first)
        def _():
            for k in range(1, nt):
                left(stat.at[0, m, t], stat_send.at[0, m, k])
            for c in range(pieces):

                @pl.when(jnp.logical_not(at_home(c)))
                def _():
                    norm_copy(m, c, True).wait_send()

        @pl.when(inner)
        def _():
            for k in range(1, nt):
                left(stat.at[1, m, t], stat_send.at[1, m, k])
            carry_copy(m).wait_send()
            for c in range(pieces):
                norm_copy(m, c, False).wait_send()

        rows_store(m).wait()
    delta_store.wait()


def run_chain(activations, targets, weight, gain_row, gain_next, dp, nt):
    tok_dev, cols = activations.shape
    depth = weight.shape[0]
    tok = tok_dev // MICRO
    pieces = cols // depth
    side = dp // 2
    bf16, f32 = jnp.bfloat16, jnp.float32
    vmem = pl.BlockSpec(memory_space=pltpu.VMEM)
    hbm = pl.BlockSpec(memory_space=pl.ANY)
    dma = pltpu.SemaphoreType.DMA
    out, residue, rows_all, delta_all = pl.pallas_call(
        chain_kernel,
        out_shape=(
            jax.ShapeDtypeStruct((tok_dev, cols), bf16),
            jax.ShapeDtypeStruct((tok_dev, 128), f32),
            jax.ShapeDtypeStruct((MICRO, dp, tok, depth), bf16),
            jax.ShapeDtypeStruct((MICRO, dp, tok, cols), bf16),
        ),
        in_specs=[vmem, vmem, hbm, vmem, vmem],
        out_specs=(vmem, vmem, hbm, hbm),
        scratch_shapes=[
            pltpu.VMEM((depth, cols), bf16),
            pltpu.VMEM((MICRO, dp, tok, depth), bf16),
            pltpu.VMEM((MICRO, dp, tok, cols), bf16),
            pltpu.VMEM((2, dp, tok, cols), f32),
            pltpu.VMEM((MICRO, side, tok, cols), bf16),
            pltpu.VMEM((MICRO, side, side, tok, cols), bf16),
            pltpu.VMEM((MICRO, tok, cols), bf16),
            pltpu.VMEM((MICRO, pieces, tok, depth), bf16),
            pltpu.VMEM((MICRO, pieces, tok, depth), bf16),
            pltpu.VMEM((2, MICRO, nt, tok, 128), f32),
            pltpu.VMEM((MICRO, dp, tok, cols), bf16),
            dma((SPLIT,)),
            dma((MICRO, dp)),
            dma((MICRO, dp, nt)),
            dma((MICRO, side)),
            dma((MICRO, SPLIT, side)),
            dma((MICRO, SPLIT, side, side)),
            dma((MICRO, SPLIT, side)),
            dma((MICRO, SPLIT, side)),
            dma((MICRO,)),
            dma((MICRO,)),
            dma((MICRO, pieces)),
            dma((MICRO, pieces)),
            dma((2, MICRO, nt)),
            dma((2, MICRO, nt)),
            dma((MICRO, dp, 2)),
            dma((MICRO, dp)),
            dma((MICRO + 1,)),
        ],
        compiler_params=pltpu.CompilerParams(has_side_effects=True, vmem_limit_bytes=VMEM_ALL),
        cost_estimate=pl.CostEstimate(
            flops=2 * tok_dev * dp * depth * cols, transcendentals=0, bytes_accessed=2 * depth * cols
        ),
    )(activations, targets, weight, gain_row, gain_next)
    return out, residue, rows_all.reshape(-1, depth), delta_all.reshape(-1, cols)


def sums_kernel(mine_ref, total_ref, held, send_sem, recv_sem):
    z, t = lax.axis_index("dp"), lax.axis_index("tensor")
    dp, nt = lax.axis_size("dp"), lax.axis_size("tensor")
    place = z * nt + t
    count = dp * nt

    def copy(k):
        peer = lax.rem(place + k, count)
        return pltpu.make_async_remote_copy(
            src_ref=mine_ref, dst_ref=held.at[place], send_sem=send_sem.at[k], recv_sem=recv_sem.at[place],
            device_id={"dp": peer // nt, "tensor": lax.rem(peer, nt)}, device_id_type=pl.DeviceIdType.MESH,
        )

    barrier = pltpu.get_barrier_semaphore()
    for k in range(1, count):
        peer = lax.rem(place + k, count)
        pl.semaphore_signal(
            barrier, inc=1, device_id={"dp": peer // nt, "tensor": lax.rem(peer, nt)},
            device_id_type=pl.DeviceIdType.MESH,
        )
    pl.semaphore_wait(barrier, count - 1)
    for k in range(1, count):
        copy(k).start()
    held[place] = mine_ref[...]
    for k in range(1, count):
        peer = lax.rem(place + k, count)
        pltpu.make_async_remote_copy(
            src_ref=mine_ref, dst_ref=held.at[peer], send_sem=send_sem.at[k], recv_sem=recv_sem.at[peer],
            device_id={"dp": z, "tensor": t}, device_id_type=pl.DeviceIdType.MESH,
        ).wait_recv()
    total = held[0]
    for k in range(1, count):
        total = total + held[k]
    total = jnp.sum(total, axis=1, keepdims=True)
    total_ref[...] = jnp.broadcast_to(jnp.sum(total, axis=2, keepdims=True), total_ref.shape)
    for k in range(1, count):
        copy(k).wait_send()


def add_sums(mine, count):
    vmem = pl.BlockSpec(memory_space=pltpu.VMEM)
    return pl.pallas_call(
        sums_kernel,
        out_shape=jax.ShapeDtypeStruct(mine.shape, mine.dtype),
        in_specs=[vmem],
        out_specs=vmem,
        scratch_shapes=[
            pltpu.VMEM((count,) + mine.shape, mine.dtype),
            pltpu.SemaphoreType.DMA((count,)),
            pltpu.SemaphoreType.DMA((count,)),
        ],
        compiler_params=pltpu.CompilerParams(has_side_effects=True, collective_id=0),
    )(mine)[:, 0, 0]


def passed_along(value, axis, steps):
    count = lax.axis_size(axis)
    leading, last = (max(0, -steps), min(count, count - steps))
    return lax.ppermute(value, axis, [(source, source + steps) for source in range(leading, last)])


def normalize(features, gain_row):
    inputs = features.astype(jnp.float32)
    mean_sq = jnp.mean(inputs * inputs, axis=1, keepdims=True)
    return (inputs * lax.rsqrt(mean_sq + norm_eps) * gain_row[None, :]).astype(jnp.bfloat16)


def ticked_chain(activations, targets, weight, gain_row):
    section_index = lax.axis_index("section")
    section_count = lax.axis_size("section")
    dp_count = lax.axis_size("dp")
    tok_dev, width_local = activations.shape
    token_total = tok_dev * dp_count
    tok_micro = tok_dev // TICKS
    received = jnp.zeros((tok_micro, width_local), jnp.bfloat16)
    row_ticks = []
    output_ticks = []
    tick_count = TICKS + section_count - 1
    for tick_index in range(tick_count):
        fed = min(tick_index, TICKS - 1) * tok_micro
        block_input = jnp.where(section_index == 0, activations[fed : fed + tok_micro], received)
        whole_rows = lax.all_gather(block_input, "tensor", axis=1, tiled=True)
        normed = normalize(whole_rows, gain_row)
        swapped = lax.all_to_all(normed, "dp", split_axis=1, concat_axis=0, tiled=True)
        partial_value = jnp.dot(swapped, weight, preferred_element_type=jnp.float32)
        branch = lax.psum_scatter(partial_value, "dp", scatter_dimension=0, tiled=True)
        block_result = (block_input.astype(jnp.float32) + branch).astype(jnp.bfloat16)
        row_ticks.append(swapped)
        output_ticks.append(block_result)
        if tick_index + 1 < tick_count:
            received = passed_along(block_result, "section", 1)
    stored_rows = lax.dynamic_slice_in_dim(jnp.stack(row_ticks), section_index, TICKS, axis=0)
    stored_rows = stored_rows.reshape(TICKS, dp_count, tok_micro, -1).transpose(1, 0, 2, 3)
    outputs_buf = lax.dynamic_slice_in_dim(
        jnp.concatenate(output_ticks), section_index * tok_micro, tok_dev, axis=0
    )
    residue = outputs_buf.astype(jnp.float32) - targets.astype(jnp.float32)
    delta = (error_scale / token_total**0.5 * residue).astype(jnp.bfloat16)
    delta_all = lax.all_gather(delta, "dp", axis=0, tiled=True)
    rows_all = stored_rows.reshape(dp_count * tok_dev, -1)
    return outputs_buf, jnp.sum(residue * residue, axis=1), rows_all, delta_all


def per_device(activations, targets, packed_floors, rounding, scales, norm_gains):
    dp_count = lax.axis_size("dp")
    core_count = lax.axis_size("tensor")
    tok_dev, width_local = activations.shape
    width_full = norm_gains.shape[1]
    token_total = tok_dev * dp_count
    weight = make_weight(packed_floors[0], rounding[0], scales)
    chained = width_local % rounding.shape[1] == 0 and dp_count % core_count == 0 and dp_count % 2 == 0
    if chained:
        here = lax.axis_index("tensor") * width_local
        gain_row = lax.dynamic_slice_in_dim(norm_gains, here, width_local, axis=1)
        gain_next = passed_along(gain_row, "section", -1)
        outputs_buf, residues, rows_all, delta_all = run_chain(
            activations, targets[0], weight, gain_row, gain_next, dp_count, core_count
        )
    else:
        outputs_buf, residues, rows_all, delta_all = ticked_chain(
            activations, targets[0], weight, norm_gains[0]
        )
    grad, sums = make_grad(rows_all, delta_all, rounding[0], scales)
    if chained:
        recon = jnp.where(lax.broadcasted_iota(jnp.int32, residues.shape, 1) == 0, residues, 0.0)
        recon = recon.reshape(-1, 8, 128).sum(axis=0)
        square_sum, penalty_sum, recon_sum = add_sums(
            jnp.concatenate([sums, recon[None]]), dp_count * core_count
        )
    else:
        recon_sum, penalty_sum, square_sum = lax.psum(
            (jnp.sum(residues), jnp.sum(sums[1]), jnp.sum(sums[0])), ("dp", "tensor")
        )
    square_sum, penalty_sum = 256.0 * square_sum, 16.0 * penalty_sum
    mean_grad = square_sum / (width_full * width_full) + grad_eps
    rounding_next = rounding[0] - (16.0 * step_rate) * grad.astype(jnp.float32) * lax.rsqrt(mean_grad)
    loss_value = recon_sum / (token_total * width_full) + reg_weight * penalty_sum / (
        width_full * width_full
    )
    return (rounding_next[None], outputs_buf[None], loss_value.reshape(1))


def solution(mesh):
    placed = (
        P("dp", "tensor"),
        P("section", "dp", "tensor"),
        P("section", "dp", "tensor"),
        P("section", "dp", "tensor"),
        P("section", "tensor"),
        P("section", None),
    )
    return jax.shard_map(
        per_device,
        mesh=mesh,
        in_specs=placed,
        out_specs=(P("section", "dp", "tensor"), P("section", "dp", "tensor"), P("section")),
        check_vma=False,
    )
```
